32 devices in a mesh: groups: 1, blk: 16 (over z, y, x), head: 2 (over core).
Axes of the slice: x: 2, y: 2, z: 4, core: 2. Of those that a mesh axis runs over, the one named last changes fastest.
Arguments:
- queries: bfloat16 [128, 8192], P(('groups', 'blk'), 'head'), may hold values from -6 to 6
- key_cache: bfloat16 [2, 32768, 8, 128], P('groups', 'blk', 'head'), may hold values from -18 to 18
- value_cache: bfloat16 [2, 32768, 8, 128], P('groups', 'blk', 'head'), may hold values from -6 to 6
- lengths: int32 [2], P('groups'), may hold values from 0 to 32704
- residual: bfloat16 [128, 8192], P('groups', 'blk'), may hold values from -6 to 6
- out_weight: bfloat16 [8192, 8192], P('head', 'blk'), may hold values from -0.0625 to 0.0625
- norm_gain: bfloat16 [8192], P('blk'), may hold values from 0.099609375 to 1.8984375
- gate_weight: bfloat16 [8192, 16384], P(None, ('head', 'blk')), may hold values from -0.0625 to 0.0625
- up_weight: bfloat16 [8192, 16384], P(None, ('head', 'blk')), may hold values from -0.0625 to 0.0625
- down_weight: bfloat16 [16384, 8192], P('head', 'blk'), may hold values from -0.046875 to 0.046875
Outputs:
- layer_out: bfloat16 [128, 8192], P('groups', 'blk')
The draws below stay inside these ranges and needn't reach their ends.
Inputs may be any that keep to these rules, and one draw needn't show every extreme that they name: lengths[b] + 64 <= 32768; the cache holds sequence b's new keys and values at positions lengths[b] to lengths[b] + 63.
All inputs are finite; a program needn't handle non-finite values.
Results may differ from the reference program's by a relative error of at most 0.01.
Values may be sent and summed in bfloat16 or wider, within the bound.
A program may use at most 128 MiB of HBM per device.

```python
import jax
import jax.numpy as jnp
from jax import lax

D = 8192
HQ = 64
KVH = 8
HD = 128
FF = 16384
B = 2
Q = 64
CTX_DEV = 2048
CTX = 32768
ROWS = 128
N_BLK = 16


def draw_queries(key, part):
    values = jnp.clip(jax.random.normal(key, (ROWS, HQ * HD), jnp.float32), -6.0, 6.0)
    return values.astype(jnp.bfloat16)


def draw_key_cache(key, part):
    values = jnp.clip(3.0 * jax.random.normal(key, (B, CTX, KVH, HD), jnp.float32), -18.0, 18.0)
    return values.astype(jnp.bfloat16)


def levels(own_key, shape, split, low, largest):
    def one(dim, parts):
        draws = jax.random.uniform(jax.random.fold_in(jax.random.fold_in(own_key, 6), dim), (parts,), jnp.float32, low / len(split), largest / len(split))
        return jnp.repeat(jnp.exp(draws), shape[dim] // parts).reshape((-1,) + (1,) * (len(shape) - dim - 1))

    gain = one(*split[0])
    for cut in split[1:]:
        gain = gain * one(*cut)
    return gain


def noise(rng, extent, deviation, bound, shards=(), kind=jnp.bfloat16):
    result = deviation * jax.random.normal(rng, extent, jnp.float32)
    if shards:
        result = result * levels(rng, extent, shards, -0.22, 0.18)
    return jnp.clip(result, -bound, bound).astype(kind)


def setup_inputs(seed: int = 0, part: int = 0) -> dict:
    splits = jax.random.split(jax.random.key(seed), 11)
    part_splits = jax.random.split(jax.random.fold_in(splits[10], part), 11)
    queries = draw_queries(jax.random.fold_in(jax.random.fold_in(splits[10], part), 71), part)
    key_cache = draw_key_cache(jax.random.fold_in(jax.random.fold_in(splits[10], part), 71), part)
    value_cache = noise(part_splits[2], (B, CTX, KVH, HD), 1.0, 6.0, ((1, 16), (2, 2)))
    lengths = jax.random.randint(part_splits[3], (B,), 0, CTX - Q + 1).astype(jnp.int32)
    residual = noise(part_splits[4], (ROWS, D), 1.0, 6.0, ((1, 16),))
    out_weight = noise(splits[5], (HQ * HD, D), (HQ * HD) ** -0.5, 0.0625, ((0, 2), (1, 16)))
    norm_gain = jnp.clip(1.0 + 0.18 * jax.random.normal(splits[6], (D,), jnp.float32), 0.099609375, 1.8984375).astype(jnp.bfloat16)
    gate_weight = noise(splits[7], (D, FF), D ** -0.5, 0.0625, ((1, 32),))
    up_weight = noise(splits[8], (D, FF), D ** -0.5, 0.0625, ((1, 32),))
    down_weight = noise(splits[9], (FF, D), FF ** -0.5, 0.046875, ((0, 2), (1, 16)))
    return {"queries": queries, "key_cache": key_cache, "value_cache": value_cache, "lengths": lengths, "residual": residual, "out_weight": out_weight, "norm_gain": norm_gain, "gate_weight": gate_weight, "up_weight": up_weight, "down_weight": down_weight}


neg_big = -1e+30
epsilon = 1e-06

def merge_stats(first, second):
    first_max, first_sum, first_out = first
    second_max, second_sum, second_out = second
    top = jnp.maximum(first_max, second_max)
    first_scale = jnp.exp(first_max - top)
    second_scale = jnp.exp(second_max - top)
    total_sum = first_sum * first_scale + second_sum * second_scale
    total_out = first_out * first_scale[..., None] + second_out * second_scale[..., None]
    return (top, total_sum, total_out)

def reference(queries, key_cache, value_cache, lengths, residual, out_weight, norm_gain, gate_weight, up_weight, down_weight):
    group_size = HQ // KVH
    shaped = queries.astype(jnp.float32).reshape(B, Q, KVH, group_size, HD)
    query_pos = lengths[:, None].astype(jnp.int32) + jnp.arange(Q, dtype=jnp.int32)[None, :]
    scale = HD ** (-0.5)

    def one_block(carry, block_index):
        first = (block_index * CTX_DEV).astype(jnp.int32)
        keys = lax.dynamic_slice_in_dim(key_cache, first, CTX_DEV, 1).astype(jnp.float32)
        values = lax.dynamic_slice_in_dim(value_cache, first, CTX_DEV, 1).astype(jnp.float32)
        key_pos = first + jnp.arange(CTX_DEV, dtype=jnp.int32)
        scores = jnp.einsum('bqkgd,bckd->bqkgc', shaped, keys) * scale
        visible = key_pos[None, None, None, None, :] <= query_pos[:, :, None, None, None]
        block_max = lax.optimization_barrier(jnp.max(jnp.where(visible, scores, neg_big), axis=-1))
        weights = jnp.where(visible, jnp.exp(scores - block_max[..., None]), 0.0)
        block_sum = lax.optimization_barrier(jnp.sum(weights, axis=-1))
        rounded = lax.optimization_barrier(weights.astype(jnp.bfloat16)).astype(jnp.float32)
        block_out = jnp.einsum('bqkgc,bckd->bqkgd', rounded, values)
        block_mean = block_out / jnp.maximum(block_sum, 1.0)[..., None]
        block_mean = lax.optimization_barrier(block_mean.astype(jnp.bfloat16)).astype(jnp.float32)
        contribution = block_mean * block_sum[..., None]
        return (merge_stats(carry, (block_max, block_sum, contribution)), None)
    start = (jnp.full((B, Q, KVH, group_size), neg_big, jnp.float32), jnp.zeros((B, Q, KVH, group_size), jnp.float32), jnp.zeros((B, Q, KVH, group_size, HD), jnp.float32))
    final, unused = lax.scan(one_block, start, jnp.arange(N_BLK, dtype=jnp.int32))
    attn = (final[2] / final[1][..., None]).astype(jnp.bfloat16).reshape(ROWS, HQ * HD)
    stream = residual.astype(jnp.float32) + jnp.dot(attn, out_weight, preferred_element_type=jnp.float32)
    squares = lax.optimization_barrier(jnp.sum(stream * stream, axis=1))
    normed = (stream * lax.rsqrt(squares / D + epsilon)[:, None] * norm_gain.astype(jnp.float32)[None, :]).astype(jnp.bfloat16)
    gate = jnp.dot(normed, gate_weight, preferred_element_type=jnp.float32)
    up = jnp.dot(normed, up_weight, preferred_element_type=jnp.float32)
    hidden = (jax.nn.silu(gate) * up).astype(jnp.bfloat16)
    down = jnp.dot(hidden, down_weight, preferred_element_type=jnp.float32)
    return (stream + down).astype(jnp.bfloat16)
```

```python
import functools
import math

import jax
import jax.numpy as jnp
from jax import lax
from jax.experimental import pallas as pl
from jax.experimental.pallas import tpu as pltpu
from jax.sharding import PartitionSpec as P

D = 8192


neg_big = -1e30
epsilon = 1e-06


def body(
    queries,
    key_cache,
    value_cache,
    lengths,
    residual,
    out_weight,
    norm_gain,
    gate_weight,
    up_weight,
    down_weight,
):
    blocks = lax.axis_size("blk")
    my_block = lax.axis_index("blk")
    batch, ctx_dev, kv_local, head_dim = key_cache.shape
    rows_dev = queries.shape[0]
    rows_all = rows_dev * blocks
    new_tokens = rows_all // batch
    heads_local = queries.shape[1] // head_dim
    group_size = heads_local // kv_local
    all_queries = lax.all_gather(queries, "blk", axis=0, tiled=True)
    shaped = all_queries.reshape(batch, new_tokens, kv_local, group_size, head_dim)
    scores = jnp.einsum(
        "bqkgd,bckd->bqkgc", shaped, key_cache, preferred_element_type=jnp.float32
    ) * head_dim ** (-0.5)
    query_pos = lengths[:, None] + jnp.arange(new_tokens, dtype=jnp.int32)[None, :]
    key_pos = my_block * ctx_dev + jnp.arange(ctx_dev, dtype=jnp.int32)
    visible = key_pos[None, None, None, None, :] <= query_pos[:, :, None, None, None]
    block_max = jnp.max(jnp.where(visible, scores, neg_big), axis=-1)
    weights = jnp.where(visible, jnp.exp(scores - block_max[..., None]), 0.0)
    block_sum = jnp.sum(weights, axis=-1)
    block_out = jnp.einsum(
        "bqkgc,bckd->bqkgd",
        weights.astype(jnp.bfloat16),
        value_cache,
        preferred_element_type=jnp.float32,
    )
    block_mean = (block_out / jnp.maximum(block_sum, 1.0)[..., None]).astype(jnp.bfloat16)
    row_max = block_max.reshape(rows_all, heads_local)
    row_sum = block_sum.reshape(rows_all, heads_local)
    row_mean = block_mean.reshape(rows_all, heads_local, head_dim)
    got_max, got_sum = (
        lax.all_to_all(row_max[None], "blk", split_axis=1, concat_axis=0, tiled=True),
        lax.all_to_all(row_sum[None], "blk", split_axis=1, concat_axis=0, tiled=True),
    )
    got_mean = lax.all_to_all(row_mean[None], "blk", split_axis=1, concat_axis=0, tiled=True)
    top = jnp.max(got_max, axis=0)
    factor = got_sum * jnp.exp(got_max - top[None])
    total_sum = jnp.sum(factor, axis=0)
    total_out = jnp.sum(got_mean.astype(jnp.float32) * factor[..., None], axis=0)
    attn = (
        (total_out / total_sum[..., None])
        .astype(jnp.bfloat16)
        .reshape(rows_dev, heads_local * head_dim)
    )
    proj_part = jnp.dot(
        lax.all_gather(attn, "blk", axis=0, tiled=True),
        out_weight,
        preferred_element_type=jnp.float32,
    )
    projected = lax.psum(proj_part.astype(jnp.bfloat16), "head").astype(jnp.float32)
    stream = residual.astype(jnp.float32) + projected
    squares = lax.psum(jnp.sum(stream * stream, axis=1), "blk")
    normed = (
        stream * lax.rsqrt(squares / D + epsilon)[:, None] * norm_gain.astype(jnp.float32)[None, :]
    ).astype(jnp.bfloat16)
    piece = lax.all_gather(normed, "blk", axis=1, tiled=True)
    gate = jnp.dot(piece, gate_weight, preferred_element_type=jnp.float32)
    up = jnp.dot(piece, up_weight, preferred_element_type=jnp.float32)
    hidden = (jax.nn.silu(gate) * up).astype(jnp.bfloat16)
    down_part = jnp.dot(
        lax.all_gather(hidden, "blk", axis=1, tiled=True),
        down_weight,
        preferred_element_type=jnp.float32,
    )
    down_total = lax.psum(down_part.astype(jnp.bfloat16), "head").astype(jnp.float32)
    return (stream + down_total).astype(jnp.bfloat16)


MESH = pl.DeviceIdType.MESH
BF = jnp.bfloat16
F32 = jnp.float32


def remote(src, dst, ssem, rsem, **where):
    return pltpu.make_async_remote_copy(
        src_ref=src, dst_ref=dst, send_sem=ssem, recv_sem=rsem, device_id=where, device_id_type=MESH
    )


def enter(n, me, head):
    barrier = pltpu.get_barrier_semaphore()
    for k in range(1, n):
        pl.semaphore_signal(
            barrier, inc=1, device_id={"blk": lax.rem(me + k, n)}, device_id_type=MESH
        )
    pl.semaphore_signal(barrier, inc=1, device_id={"head": 1 - head}, device_id_type=MESH)
    pl.semaphore_wait(barrier, n)


def start_if(cond, copy):
    if cond is None:
        copy.start()
    else:
        pl.when(cond)(copy.start)


def gather(buf, parts, ssem, rsem, n, me, forward=None):
    depth = n // 4
    z = me // 4
    x_peer = me + 1 - 2 * (me % 2)
    y_peer = me + 2 - 4 * ((me // 2) % 2)
    sends = []

    def send(part, slot, block, target, cond=None):
        copy = remote(
            buf.at[part, block], buf.at[part, block], ssem.at[part, slot], rsem.at[part, block], blk=target
        )
        start_if(cond, copy)
        sends.append((cond, copy))

    def pass_on(part, block, cond=None):
        if forward is not None:
            head, fsem = forward
            copy = remote(
                buf.at[part, block], buf.at[part, block], fsem.at[block], rsem.at[part, block], head=1 - head
            )
            start_if(cond, copy)
            sends.append((cond, copy))

    def arrived(part, block, cond=None):
        copy = remote(
            buf.at[part, block], buf.at[part, block], ssem.at[part, 0], rsem.at[part, block], blk=x_peer
        )
        if cond is None:
            copy.wait_recv()
        else:
            pl.when(cond)(copy.wait_recv)

    def peers(first):
        return x_peer * (1 - first) + y_peer * first, y_peer * (1 - first) + x_peer * first

    for part, first in parts:
        near, far = peers(first)
        send(part, 0, me, me + 4, z < depth - 1)
        send(part, 1, me, me - 4, z > 0)
        send(part, 2, me, near)
        send(part, 3, me, far)
        pass_on(part, me)
    slot = 4
    for d in range(1, depth):
        for step in (4, -4):
            for part, first in parts:
                near, far = peers(first)
                block = me - step * d
                if step > 0:
                    here = z >= d
                    more = jnp.logical_and(z >= d, z < depth - 1)
                else:
                    here = z < depth - d
                    more = jnp.logical_and(z < depth - d, z > 0)
                arrived(part, block, here)
                send(part, slot, block, me + step, more)
                send(part, slot + 1, block, near, here)
                send(part, slot + 2, block, far, here)
                pass_on(part, block, here)
            slot += 3
    for k in range(depth):
        zz = lax.rem(z + k, depth)
        for part, first in parts:
            near, far = peers(first)
            block = near + 4 * (zz - z)
            arrived(part, block)
            send(part, slot, block, far)
            pass_on(part, block)
        slot += 1
    for k in range(depth):
        zz = lax.rem(z + k, depth)
        for part, first in parts:
            near, far = peers(first)
            for block in (far + 4 * (zz - z), near + far - me + 4 * (zz - z)):
                arrived(part, block)
                pass_on(part, block)
    if forward is not None:
        head = forward[0]
        for i in range(n):
            arrived(1 - head, i)

    def finish():
        for cond, copy in sends:
            if cond is None:
                copy.wait_send()
            else:
                pl.when(cond)(copy.wait_send)

    return finish


def slots(n):
    depth = n // 4
    return 4 + 6 * (depth - 1) + depth


def swap(part, mine, theirs, ssem, rsem, head):
    mine[...] = part.astype(BF)
    copy = remote(mine, theirs, ssem, rsem, head=1 - head)
    copy.start()
    copy.wait()
    return mine[...].astype(F32) + theirs[...].astype(F32)


def attend(
    n, lengths, q, keys, values, residual, gain, ow,
    stream_out, scaled_out, squares_out,
    qbuf, kraw, vraw, wide, kd, vd, qs, osend, orecv, stat, statr, abuf, ow_v, acc, mine, theirs,
    qss, qrs, oss, ors, tss, trs, ass, ars, loc, xss, xrs,
):
    me = lax.axis_index("blk")
    head = lax.axis_index("head")
    batch, flat, hd = kraw.shape
    kv = kd.shape[0] // batch
    ctx = flat // kv
    rows_dev, width = q.shape
    half = width // 2
    per = half // hd
    group = width // hd // kv
    owners = n // batch
    tokens = owners * rows_dev
    kcopy = pltpu.make_async_copy(keys, kraw, loc.at[0])
    vcopy = pltpu.make_async_copy(values, vraw, loc.at[1])
    wcopy = pltpu.make_async_copy(ow, ow_v, loc.at[2])
    qcopies = [
        pltpu.make_async_copy(q.at[:, pl.ds(p * half, half)], qbuf.at[p, me], loc.at[3 + p])
        for p in range(2)
    ]
    for c in qcopies:
        c.start()
    kcopy.start()
    vcopy.start()
    wcopy.start()
    enter(n, me, head)
    for c in qcopies:
        c.wait()
    finish_q = gather(qbuf, [(0, 0), (1, 1)], qss, qrs, n, me)
    kcopy.wait()
    vcopy.wait()
    for raw, out in ((kraw, kd), (vraw, vd)):
        for b in range(batch):
            wide[...] = raw[b].astype(F32)
            for h in range(kv):
                out[b * kv + h] = wide[pl.ds(h, ctx, stride=kv), :].astype(BF)
    for b in range(batch):
        for j in range(kv * group):
            val = qbuf[j // per, b * owners : (b + 1) * owners, :, (j % per) * hd : (j % per + 1) * hd]
            val = val.astype(F32).reshape(tokens, hd).astype(BF)
            h, g = j // group, j % group
            qs[b * kv + h, g * tokens : (g + 1) * tokens] = val
    scale = hd ** (-0.5) * math.log2(math.e)
    gt = 4
    tile = gt * tokens
    lane = lax.broadcasted_iota(jnp.int32, (owners, rows_dev, 128), 2)

    def one(bh, carry):
        b, h = bh // kv, bh % kv
        limit = lengths[b] - me * ctx
        for rt in range(group // gt):
            s = lax.dot_general(
                qs[bh, rt * tile : (rt + 1) * tile], kd[bh], (((1,), (1,)), ((), ())), preferred_element_type=F32
            ) * scale
            row = lax.broadcasted_iota(jnp.int32, (tile, 1), 0) % tokens
            col = lax.broadcasted_iota(jnp.int32, (tile, ctx), 1)
            s = jnp.where(col <= row + limit, s, neg_big)
            m = jnp.max(s, axis=1, keepdims=True)
            p = jnp.exp2(s - jnp.maximum(m, -1e29))
            l = jnp.sum(p, axis=1, keepdims=True)
            o = jnp.dot(p.astype(BF), vd[bh], preferred_element_type=F32)
            o = o / jnp.maximum(l, 1.0)
            for g in range(gt):
                gg = rt * gt + g
                cut = slice(g * tokens, (g + 1) * tokens)
                piece = o[cut].reshape(owners, rows_dev, hd).astype(BF)
                osend[h, pl.ds(b * owners, owners), :, gg * hd : (gg + 1) * hd] = piece
                at = h * group + gg
                for which, col_value in ((0, m), (1, l)):
                    old = stat[pl.ds(b * owners, owners), which]
                    new = jnp.broadcast_to(col_value[cut], (tokens, 128)).reshape(owners, rows_dev, 128)
                    stat[pl.ds(b * owners, owners), which] = jnp.where(lane == at, new, old)
        for j in range(owners):
            to = b * owners + j
            copy = remote(osend.at[h, to], orecv.at[h, me], oss.at[h, to], ors.at[h, me], blk=to)
            start_if(to != me, copy)
        return carry

    stat[...] = jnp.zeros_like(stat)
    lax.fori_loop(0, batch * kv, one, 0)
    for to in range(n):
        start_if(to != me, remote(stat.at[to], statr.at[me], tss.at[to], trs.at[me], blk=to))
    own = [pltpu.make_async_copy(stat.at[me], statr.at[me], loc.at[3])]
    own += [pltpu.make_async_copy(osend.at[h, me], orecv.at[h, me], loc.at[5 + h]) for h in range(kv)]
    for c in own:
        c.start()
    finish_q()
    for c in own:
        c.wait()
    for i in range(n):
        for h in range(kv):
            copy = remote(osend.at[h, i], orecv.at[h, i], oss.at[h, i], ors.at[h, i], blk=i)
            pl.when(i != me)(copy.wait)
        pl.when(i != me)(remote(stat.at[i], statr.at[i], tss.at[i], trs.at[i], blk=i).wait)
    maxima = statr[:, 0]
    top = jnp.max(maxima, axis=0)
    factor = statr[:, 1] * jnp.exp2(maxima - top[None])
    total = jnp.sum(factor, axis=0)
    for j in range(kv * group):
        h, g = j // group, j % group
        out = jnp.sum(
            orecv[h, :, :, g * hd : (g + 1) * hd].astype(F32) * factor[:, :, j : j + 1], axis=0
        ) / total[:, j : j + 1]
        abuf[j // per, me, :, (j % per) * hd : (j % per + 1) * hd] = out.astype(BF)
    finish_a = gather(abuf, [(0, 0), (1, 1)], ass, ars, n, me)
    wcopy.wait()
    acc[...] = jnp.zeros_like(acc)
    chunk = 512
    for p in range(2):
        def proj(c, carry, p=p):
            at = pl.multiple_of(c * chunk, chunk)
            lhs = abuf[p, :, :, pl.ds(at, chunk)].astype(F32).reshape(n * rows_dev, chunk).astype(BF)
            acc[...] += jnp.dot(lhs, ow_v[pl.ds(p * half + at, chunk), :], preferred_element_type=F32)
            return carry
        lax.fori_loop(0, half // chunk, proj, 0)
    finish_a()
    stream = residual[...].astype(F32) + swap(acc[...], mine, theirs, xss, xrs, head)
    stream_out[...] = stream
    scaled = (stream * gain[...].astype(F32)).astype(BF)
    cut = scaled.shape[1] // 2
    scaled_out[0] = scaled[:, :cut]
    scaled_out[1] = scaled[:, cut:]
    squares_out[...] = lax.dot_general(
        jnp.ones((8, stream.shape[1]), F32), stream * stream, (((1,), (1,)), ((), ())),
        precision=lax.Precision.HIGHEST, preferred_element_type=F32,
    )


def feed(
    n, stream, scaled, squares, gw, uw, dw, out,
    sbuf, sqbuf, hbuf, gv, uv, dv, gacc, uacc, mine, theirs,
    sss, srs, sfs, qss, qrs, hss, hrs, loc, xss, xrs,
):
    me = lax.axis_index("blk")
    head = lax.axis_index("head")
    weights = [pltpu.make_async_copy(a, b, loc.at[i]) for i, (a, b) in enumerate(((gw, gv), (uw, uv), (dw, dv)))]
    own = pltpu.make_async_copy(scaled.at[head], sbuf.at[head, me], loc.at[3])
    own_sq = pltpu.make_async_copy(squares, sqbuf.at[me], loc.at[4])
    own.start()
    own_sq.start()
    for c in weights:
        c.start()
    enter(n, me, head)
    own.wait()
    own_sq.wait()
    for i in range(n):
        start_if(i != me, remote(sqbuf.at[me], sqbuf.at[me], qss.at[i], qrs.at[me], blk=i))
    finish_s = gather(sbuf, [(head, head)], sss, srs, n, me, forward=(head, sfs))
    for i in range(n):
        pl.when(i != me)(remote(sqbuf.at[i], sqbuf.at[i], qss.at[i], qrs.at[i], blk=i).wait)
    cut = sbuf.shape[3]
    unroll = 4

    def product(buf, pairs):
        for acc, _ in pairs:
            acc[...] = jnp.zeros_like(acc)

        def step(c, carry):
            for acc, w in pairs:
                total = None
                for k in range(unroll):
                    for p in range(2):
                        i = c * unroll + k
                        at = pl.multiple_of(i * 2 * cut + p * cut, cut)
                        term = jnp.dot(buf[p, i], w[pl.ds(at, cut), :], preferred_element_type=F32)
                        total = term if total is None else total + term
                acc[...] += total
            return carry

        lax.fori_loop(0, n // unroll, step, 0)

    weights[0].wait()
    weights[1].wait()
    product(sbuf, ((gacc, gv), (uacc, uv)))
    total = jnp.sum(sqbuf[...], axis=0)
    width = gacc.shape[1]
    spread = lax.dot_general(
        total, jnp.full((8, width), 0.125, F32), (((0,), (0,)), ((), ())),
        precision=lax.Precision.HIGHEST, preferred_element_type=F32,
    )
    scale = lax.rsqrt(spread / (n * stream.shape[1]) + epsilon)
    gate = gacc[...] * scale
    hidden = ((gate / (1.0 + jnp.exp(-gate))) * (uacc[...] * scale)).astype(BF)
    hbuf[0, me] = hidden[:, :cut]
    hbuf[1, me] = hidden[:, cut:]
    finish_h = gather(hbuf, [(0, 0), (1, 1)], hss, hrs, n, me)
    weights[2].wait()
    product(hbuf, ((gacc, dv),))
    out[...] = (stream[...] + swap(gacc[...], mine, theirs, xss, xrs, head)).astype(BF)
    finish_s()
    finish_h()


VM = pl.BlockSpec(memory_space=pltpu.VMEM)
HBM = pl.BlockSpec(memory_space=pl.ANY)
DMA = pltpu.SemaphoreType.DMA


def kernel_body(
    queries, key_cache, value_cache, lengths, residual, out_weight, norm_gain, gate_weight, up_weight, down_weight
):
    n = lax.axis_size("blk")
    batch, ctx, kv, hd = key_cache.shape
    rows_dev, width = queries.shape
    half = width // 2
    group = width // hd // kv
    rows, cols = residual.shape
    keys = key_cache.reshape(batch, ctx * kv, hd)
    values = value_cache.reshape(batch, ctx * kv, hd)
    block = (n, rows_dev, group * hd)
    s = slots(n)
    stream, scaled, squares = pl.pallas_call(
        functools.partial(attend, n),
        out_shape=(
            jax.ShapeDtypeStruct((rows, cols), F32),
            jax.ShapeDtypeStruct((2, rows, cols // 2), BF),
            jax.ShapeDtypeStruct((8, rows), F32),
        ),
        in_specs=[pl.BlockSpec(memory_space=pltpu.SMEM), VM, HBM, HBM, VM, VM, HBM],
        out_specs=(VM, VM, VM),
        scratch_shapes=[
            pltpu.VMEM((2, n, rows_dev, half), BF),
            pltpu.VMEM(keys.shape, BF),
            pltpu.VMEM(keys.shape, BF),
            pltpu.VMEM(keys.shape[1:], F32),
            pltpu.VMEM((batch * kv, ctx, hd), BF),
            pltpu.VMEM((batch * kv, ctx, hd), BF),
            pltpu.VMEM((batch * kv, group * rows // batch, hd), BF),
            pltpu.VMEM((kv,) + block, BF),
            pltpu.VMEM((kv,) + block, BF),
            pltpu.VMEM((n, 2, rows_dev, 128), F32),
            pltpu.VMEM((n, 2, rows_dev, 128), F32),
            pltpu.VMEM((2, n, rows_dev, half), BF),
            pltpu.VMEM(out_weight.shape, BF),
            pltpu.VMEM((rows, cols), F32),
            pltpu.VMEM((rows, cols), BF),
            pltpu.VMEM((rows, cols), BF),
            DMA((2, s)), DMA((2, n)), DMA((kv, n)), DMA((kv, n)), DMA((n,)), DMA((n,)),
            DMA((2, s)), DMA((2, n)), DMA((5 + kv,)), DMA, DMA,
        ],
        compiler_params=pltpu.CompilerParams(
            collective_id=0, has_side_effects=True, vmem_limit_bytes=60 * 1024 * 1024
        ),
        name="attend",
    )(lengths, queries, keys, values, residual, norm_gain.reshape(1, -1), out_weight)
    units = gate_weight.shape[1]
    return pl.pallas_call(
        functools.partial(feed, n),
        out_shape=jax.ShapeDtypeStruct((rows, cols), BF),
        in_specs=[VM, VM, VM, HBM, HBM, HBM],
        out_specs=VM,
        scratch_shapes=[
            pltpu.VMEM((2, n, rows, cols // 2), BF),
            pltpu.VMEM((n, 8, rows), F32),
            pltpu.VMEM((2, n, rows, units // 2), BF),
            pltpu.VMEM(gate_weight.shape, BF),
            pltpu.VMEM(up_weight.shape, BF),
            pltpu.VMEM(down_weight.shape, BF),
            pltpu.VMEM((rows, units), F32),
            pltpu.VMEM((rows, units), F32),
            pltpu.VMEM((rows, cols), BF),
            pltpu.VMEM((rows, cols), BF),
            DMA((2, s)), DMA((2, n)), DMA((n,)), DMA((n,)), DMA((n,)),
            DMA((2, s)), DMA((2, n)), DMA((5,)), DMA, DMA,
        ],
        compiler_params=pltpu.CompilerParams(
            collective_id=1, has_side_effects=True, vmem_limit_bytes=60 * 1024 * 1024
        ),
        name="feed",
    )(stream, scaled, squares, gate_weight, up_weight, down_weight)


def pick(*args):
    queries, key_cache, residual, gate_weight = args[0], args[1], args[4], args[7]
    n = lax.axis_size("blk")
    fits = (
        n % 8 == 0
        and queries.shape[0] == 8
        and n % key_cache.shape[0] == 0
        and residual.shape[1] % 256 == 0
        and residual.shape[1] == gate_weight.shape[1]
        and residual.shape[0] == 128
    )
    return kernel_body(*args) if fits else body(*args)


def solution(mesh):
    in_specs = (
        P(("groups", "blk"), "head"),
        P("groups", "blk", "head", None),
        P("groups", "blk", "head", None),
        P("groups"),
        P("groups", "blk"),
        P("head", "blk"),
        P("blk"),
        P(None, ("head", "blk")),
        P(None, ("head", "blk")),
        P("head", "blk"),
    )
    out_specs = P("groups", "blk")
    return jax.shard_map(pick, mesh=mesh, in_specs=in_specs, out_specs=out_specs, check_vma=False)
```

```python
import functools
import math

import jax
import jax.numpy as jnp
from jax import lax
from jax.experimental import pallas as pl
from jax.experimental.pallas import tpu as pltpu
from jax.sharding import PartitionSpec as P

D = 8192


neg_big = -1e30
epsilon = 1e-06


def body(
    queries,
    key_cache,
    value_cache,
    lengths,
    residual,
    out_weight,
    norm_gain,
    gate_weight,
    up_weight,
    down_weight,
):
    blocks = lax.axis_size("blk")
    my_block = lax.axis_index("blk")
    batch, ctx_dev, kv_local, head_dim = key_cache.shape
    rows_dev = queries.shape[0]
    rows_all = rows_dev * blocks
    new_tokens = rows_all // batch
    heads_local = queries.shape[1] // head_dim
    group_size = heads_local // kv_local
    all_queries = lax.all_gather(queries, "blk", axis=0, tiled=True)
    shaped = all_queries.reshape(batch, new_tokens, kv_local, group_size, head_dim)
    scores = jnp.einsum(
        "bqkgd,bckd->bqkgc", shaped, key_cache, preferred_element_type=jnp.float32
    ) * head_dim ** (-0.5)
    query_pos = lengths[:, None] + jnp.arange(new_tokens, dtype=jnp.int32)[None, :]
    key_pos = my_block * ctx_dev + jnp.arange(ctx_dev, dtype=jnp.int32)
    visible = key_pos[None, None, None, None, :] <= query_pos[:, :, None, None, None]
    block_max = jnp.max(jnp.where(visible, scores, neg_big), axis=-1)
    weights = jnp.where(visible, jnp.exp(scores - block_max[..., None]), 0.0)
    block_sum = jnp.sum(weights, axis=-1)
    block_out = jnp.einsum(
        "bqkgc,bckd->bqkgd",
        weights.astype(jnp.bfloat16),
        value_cache,
        preferred_element_type=jnp.float32,
    )
    block_mean = (block_out / jnp.maximum(block_sum, 1.0)[..., None]).astype(jnp.bfloat16)
    row_max = block_max.reshape(rows_all, heads_local)
    row_sum = block_sum.reshape(rows_all, heads_local)
    row_mean = block_mean.reshape(rows_all, heads_local, head_dim)
    got_max, got_sum = (
        lax.all_to_all(row_max[None], "blk", split_axis=1, concat_axis=0, tiled=True),
        lax.all_to_all(row_sum[None], "blk", split_axis=1, concat_axis=0, tiled=True),
    )
    got_mean = lax.all_to_all(row_mean[None], "blk", split_axis=1, concat_axis=0, tiled=True)
    top = jnp.max(got_max, axis=0)
    factor = got_sum * jnp.exp(got_max - top[None])
    total_sum = jnp.sum(factor, axis=0)
    total_out = jnp.sum(got_mean.astype(jnp.float32) * factor[..., None], axis=0)
    attn = (
        (total_out / total_sum[..., None])
        .astype(jnp.bfloat16)
        .reshape(rows_dev, heads_local * head_dim)
    )
    proj_part = jnp.dot(
        lax.all_gather(attn, "blk", axis=0, tiled=True),
        out_weight,
        preferred_element_type=jnp.float32,
    )
    projected = lax.psum(proj_part.astype(jnp.bfloat16), "head").astype(jnp.float32)
    stream = residual.astype(jnp.float32) + projected
    squares = lax.psum(jnp.sum(stream * stream, axis=1), "blk")
    normed = (
        stream * lax.rsqrt(squares / D + epsilon)[:, None] * norm_gain.astype(jnp.float32)[None, :]
    ).astype(jnp.bfloat16)
    piece = lax.all_gather(normed, "blk", axis=1, tiled=True)
    gate = jnp.dot(piece, gate_weight, preferred_element_type=jnp.float32)
    up = jnp.dot(piece, up_weight, preferred_element_type=jnp.float32)
    hidden = (jax.nn.silu(gate) * up).astype(jnp.bfloat16)
    down_part = jnp.dot(
        lax.all_gather(hidden, "blk", axis=1, tiled=True),
        down_weight,
        preferred_element_type=jnp.float32,
    )
    down_total = lax.psum(down_part.astype(jnp.bfloat16), "head").astype(jnp.float32)
    return (stream + down_total).astype(jnp.bfloat16)


MESH = pl.DeviceIdType.MESH
BF = jnp.bfloat16
F32 = jnp.float32


def remote(src, dst, ssem, rsem, **where):
    return pltpu.make_async_remote_copy(
        src_ref=src, dst_ref=dst, send_sem=ssem, recv_sem=rsem, device_id=where, device_id_type=MESH
    )


def enter(n, me, head):
    barrier = pltpu.get_barrier_semaphore()
    for k in range(1, n):
        pl.semaphore_signal(
            barrier, inc=1, device_id={"blk": lax.rem(me + k, n)}, device_id_type=MESH
        )
    pl.semaphore_signal(barrier, inc=1, device_id={"head": 1 - head}, device_id_type=MESH)
    pl.semaphore_wait(barrier, n)


def start_if(cond, copy):
    if cond is None:
        copy.start()
    else:
        pl.when(cond)(copy.start)


def gather(buf, parts, ssem, rsem, n, me, forward=None, work=(), visit=None):
    depth = n // 4
    z = me // 4
    x_peer = me + 1 - 2 * (me % 2)
    y_peer = me + 2 - 4 * ((me // 2) % 2)
    sends = []

    def send(part, slot, block, target, cond=None):
        copy = remote(
            buf.at[part, block], buf.at[part, block], ssem.at[part, slot], rsem.at[part, block], blk=target
        )
        start_if(cond, copy)
        sends.append((cond, copy))

    def pass_on(part, block, cond=None):
        if forward is not None:
            head, fsem = forward
            copy = remote(
                buf.at[part, block], buf.at[part, block], fsem.at[block], rsem.at[part, block], head=1 - head
            )
            start_if(cond, copy)
            sends.append((cond, copy))

    def arrived(part, block, cond=None):
        copy = remote(
            buf.at[part, block], buf.at[part, block], ssem.at[part, 0], rsem.at[part, block], blk=x_peer
        )
        if cond is None:
            copy.wait_recv()
        else:
            pl.when(cond)(copy.wait_recv)

    def peers(first):
        return x_peer * (1 - first) + y_peer * first, y_peer * (1 - first) + x_peer * first

    for part, first in parts:
        near, far = peers(first)
        send(part, 0, me, me + 4, z < depth - 1)
        send(part, 1, me, me - 4, z > 0)
        send(part, 2, me, near)
        send(part, 3, me, far)
        pass_on(part, me)
    work = list(work)
    if work:
        work.pop(0)()
    slot = 4
    for d in range(1, depth):
        for step in (4, -4):
            for part, first in parts:
                near, far = peers(first)
                block = me - step * d
                if step > 0:
                    here = z >= d
                    more = jnp.logical_and(z >= d, z < depth - 1)
                else:
                    here = z < depth - d
                    more = jnp.logical_and(z < depth - d, z > 0)
                arrived(part, block, here)
                send(part, slot, block, me + step, more)
                send(part, slot + 1, block, near, here)
                send(part, slot + 2, block, far, here)
                pass_on(part, block, here)
            slot += 3
        if work:
            work.pop(0)()
    for k in range(depth):
        zz = lax.rem(z + k, depth)
        for part, first in parts:
            near, far = peers(first)
            block = near + 4 * (zz - z)
            arrived(part, block)
            send(part, slot, block, far)
            pass_on(part, block)
        slot += 1
    if work:
        work.pop(0)()
    others = [] if forward is None else [(1 - p, 1 - f) for p, f in parts]
    for group in (parts, others):
        items = []
        for k in range(depth):
            shift = 4 * (lax.rem(z + k, depth) - z)
            for part, first in group:
                near, far = peers(first)
                if group is others:
                    arrived(part, me + shift)
                    arrived(part, near + shift)
                items += [(part, me + shift), (part, near + shift)]
        if visit is not None and items:
            visit(items)
    for k in range(depth):
        shift = 4 * (lax.rem(z + k, depth) - z)
        items = []
        for mine, (part, first) in [(True, p) for p in parts] + [(False, p) for p in others]:
            near, far = peers(first)
            for block in (far + shift, near + far - me + shift):
                arrived(part, block)
                if mine:
                    pass_on(part, block)
                items.append((part, block))
        if visit is not None:
            visit(items)

    def finish():
        for cond, copy in sends:
            if cond is None:
                copy.wait_send()
            else:
                pl.when(cond)(copy.wait_send)

    return finish


def slots(n):
    depth = n // 4
    return 4 + 6 * (depth - 1) + depth


def swap(part, mine, theirs, ssem, rsem, head):
    mine[...] = part.astype(BF)
    copy = remote(mine, theirs, ssem, rsem, head=1 - head)
    copy.start()
    copy.wait()
    return mine[...].astype(F32) + theirs[...].astype(F32)


def layer(
    n, lengths, q, keys, values, residual, gain, ow, gw, uw, dw, out,
    qbuf, raw, wide, kd, vd, qs, osend, orecv, stat, ssend, srecv, abuf, sbuf, sqbuf, hbuf,
    ow_v, gv, uv, dv, stream, acc, gacc, mine, theirs,
    qss, qrs, oss, ors, tss, trs, ass, ars, sss, srs, sfs, nss, nrs, hss, hrs, loc, wsem, xss, xrs,
):
    me = lax.axis_index("blk")
    head = lax.axis_index("head")
    batch, flat, hd = raw.shape
    kv = kd.shape[0] // batch
    ctx = flat // kv
    rows_dev, width = q.shape
    half = width // 2
    per = half // hd
    group = width // hd // kv
    owners = n // batch
    tokens = owners * rows_dev
    rows = batch * tokens
    wcopies = [
        pltpu.make_async_copy(a, b, wsem.at[i])
        for i, (a, b) in enumerate(((ow, ow_v), (gw, gv), (uw, uv), (dw, dv)))
    ]
    qcopies = [
        pltpu.make_async_copy(q.at[:, pl.ds(p * half, half)], qbuf.at[p, me], loc.at[p]) for p in range(2)
    ]
    for c in qcopies:
        c.start()
    kcopies = [pltpu.make_async_copy(keys.at[b], raw.at[b], loc.at[2 + b]) for b in range(batch)]
    vcopies = [pltpu.make_async_copy(values.at[b], raw.at[b], loc.at[2 + b]) for b in range(batch)]
    for c in kcopies:
        c.start()
    enter(n, me, head)
    for c in qcopies:
        c.wait()

    def spread_heads(dest, b, copies, after):
        def run():
            copies[b].wait()
            part = wide.shape[0]
            for c in range(flat // part):
                wide[...] = raw[b, c * part : (c + 1) * part].astype(F32)
                for h in range(kv):
                    dest[b * kv + h, c * part // kv : (c + 1) * part // kv] = wide[
                        pl.ds(h, part // kv, stride=kv), :
                    ].astype(BF)
            for c in after:
                c.start()
        return run

    jobs = []
    for b in range(batch):
        jobs.append(spread_heads(kd, b, kcopies, [vcopies[b]]))
    for b in range(batch):
        jobs.append(spread_heads(vd, b, vcopies, wcopies if b == batch - 1 else []))
    finish_q = gather(qbuf, [(0, 0), (1, 1)], qss, qrs, n, me, work=jobs)
    for b in range(batch):
        for j in range(kv * group):
            val = qbuf[j // per, b * owners : (b + 1) * owners, :, (j % per) * hd : (j % per + 1) * hd]
            val = val.astype(F32).reshape(tokens, hd).astype(BF)
            h, g = j // group, j % group
            qs[b * kv + h, g * tokens : (g + 1) * tokens] = val
    scale = hd ** (-0.5) * math.log2(math.e)
    gt = 4
    tile = gt * tokens
    share = n // kv
    heads_each = group // share
    lane = lax.broadcasted_iota(jnp.int32, (tokens, 128), 1)
    z = me // 4

    def one(b, h):
        bh = b * kv + h
        limit = lengths[b] - me * ctx
        first_row = pl.multiple_of(b * tokens, tokens)
        stats = jnp.zeros((tokens, 128), F32)
        for rt in range(group // gt):
            s = lax.dot_general(
                qs[bh, rt * tile : (rt + 1) * tile], kd[bh], (((1,), (1,)), ((), ())), preferred_element_type=F32
            ) * scale
            row = lax.broadcasted_iota(jnp.int32, (tile, 1), 0) % tokens
            col = lax.broadcasted_iota(jnp.int32, (tile, ctx), 1)
            s = jnp.where(col <= row + limit, s, neg_big)
            m = jnp.max(s, axis=1, keepdims=True)
            p = jnp.exp2(s - jnp.maximum(m, -1e29))
            l = jnp.sum(p, axis=1, keepdims=True)
            o = jnp.dot(p.astype(BF), vd[bh], preferred_element_type=F32)
            o = (o / jnp.maximum(l, 1.0)).astype(BF)
            for g in range(gt):
                j, e = divmod(rt * gt + g, heads_each)
                cut = slice(g * tokens, (g + 1) * tokens)
                osend[h * share + j, pl.ds(first_row, tokens), e * hd : (e + 1) * hd] = o[cut]
                stats = jnp.where(lane == j * 8 + e, m[cut], stats)
                stats = jnp.where(lane == 64 + j * 8 + e, l[cut], stats)
            for j in range(rt * gt // heads_each, (rt + 1) * gt // heads_each):
                to = h * share + j
                copy = remote(
                    osend.at[to, pl.ds(first_row, tokens)], orecv.at[me, pl.ds(first_row, tokens)],
                    oss.at[b, to], ors.at[b, me], blk=to,
                )
                start_if(to != me, copy)
        stat[pl.ds(first_row, tokens)] = stats

    def plane(k, carry):
        h = lax.rem(z + kv - 1 - k, kv)

        def each(b, c):
            one(b, h)
            return c

        lax.fori_loop(0, batch, each, 0)
        turned = stat[...].T
        for j in range(share):
            to = h * share + j
            for which in range(2):
                ssend[to, which] = turned[which * 64 + j * 8 : which * 64 + j * 8 + 8]
            start_if(to != me, remote(ssend.at[to], srecv.at[me], tss.at[to], trs.at[me], blk=to))
        return carry

    lax.fori_loop(0, kv, plane, 0)
    own = [
        pltpu.make_async_copy(ssend.at[me], srecv.at[me], loc.at[0]),
        pltpu.make_async_copy(osend.at[me], orecv.at[me], loc.at[1]),
    ]
    for c in own:
        c.start()
    finish_q()
    for c in own:
        c.wait()
    for i in range(n):
        for b in range(batch):
            cut = pl.ds(b * tokens, tokens)
            copy = remote(osend.at[i, cut], orecv.at[i, cut], oss.at[b, i], ors.at[b, i], blk=i)
            pl.when(i != me)(copy.wait)
        pl.when(i != me)(remote(ssend.at[i], srecv.at[i], tss.at[i], trs.at[i], blk=i).wait)
    maxima = srecv[:, 0]
    top = jnp.max(maxima, axis=0)
    factor = srecv[:, 1] * jnp.exp2(maxima - top[None])
    ratio = (factor / jnp.sum(factor, axis=0)[None]).reshape(n * 8, rows).T
    for e in range(heads_each):
        total = jnp.zeros((rows, hd), F32)
        for i in range(n):
            total += orecv[i, :, e * hd : (e + 1) * hd].astype(F32) * ratio[:, i * 8 + e : i * 8 + e + 1]
        abuf[e, me] = total.astype(BF)

    def products(buf, pairs):
        cut = buf.shape[3]

        def visit(items):
            for c in range(0, len(items), 4):
                for total, w in pairs:
                    term = total[...]
                    for part, block in items[c : c + 4]:
                        at = pl.multiple_of(block * (2 * cut) + part * cut, cut)
                        term += jnp.dot(buf[part, block], w[pl.ds(at, cut), :], preferred_element_type=F32)
                    total[...] = term
        return visit

    acc[...] = jnp.zeros_like(acc)
    for c in wcopies:
        c.wait()
    finish_a = gather(abuf, [(0, 0), (1, 1)], ass, ars, n, me, visit=products(abuf, ((acc, ow_v),)))
    new = residual[...].astype(F32) + swap(acc[...], mine.at[0], theirs.at[0], xss.at[0], xrs.at[0], head)
    stream[...] = new
    scaled = (new * gain[...].astype(F32)).astype(BF)
    cut = scaled.shape[1] // 2
    for p in range(2):
        @pl.when(head == p)
        def _(p=p):
            sbuf[p, me] = scaled[:, p * cut : (p + 1) * cut]
    sqbuf[me] = lax.dot_general(
        jnp.ones((8, new.shape[1]), F32), new * new, (((1,), (1,)), ((), ())),
        precision=lax.Precision.HIGHEST, preferred_element_type=F32,
    )
    acc[...] = jnp.zeros_like(acc)
    gacc[...] = jnp.zeros_like(gacc)
    for i in range(n):
        start_if(i != me, remote(sqbuf.at[me], sqbuf.at[me], nss.at[i], nrs.at[me], blk=i))
    finish_s = gather(
        sbuf, [(head, head)], sss, srs, n, me, forward=(head, sfs),
        visit=products(sbuf, ((gacc, gv), (acc, uv))),
    )
    for i in range(n):
        pl.when(i != me)(remote(sqbuf.at[i], sqbuf.at[i], nss.at[i], nrs.at[i], blk=i).wait)
    spread = lax.dot_general(
        jnp.sum(sqbuf[...], axis=0), jnp.full((8, gacc.shape[1]), 0.125, F32), (((0,), (0,)), ((), ())),
        precision=lax.Precision.HIGHEST, preferred_element_type=F32,
    )
    norm = lax.rsqrt(spread / (n * stream.shape[1]) + epsilon)
    gate = gacc[...] * norm
    hidden = ((gate / (1.0 + jnp.exp(-gate))) * (acc[...] * norm)).astype(BF)
    cut = hidden.shape[1] // 2
    hbuf[0, me] = hidden[:, :cut]
    hbuf[1, me] = hidden[:, cut:]
    acc[...] = jnp.zeros_like(acc)
    finish_h = gather(hbuf, [(0, 0), (1, 1)], hss, hrs, n, me, visit=products(hbuf, ((acc, dv),)))
    down = swap(acc[...], mine.at[1], theirs.at[1], xss.at[1], xrs.at[1], head)
    out[...] = (stream[...] + down).astype(BF)
    finish_a()
    finish_s()
    finish_h()


VM = pl.BlockSpec(memory_space=pltpu.VMEM)
HBM = pl.BlockSpec(memory_space=pl.ANY)
DMA = pltpu.SemaphoreType.DMA


def kernel_body(
    queries, key_cache, value_cache, lengths, residual, out_weight, norm_gain, gate_weight, up_weight, down_weight
):
    n = lax.axis_size("blk")
    batch, ctx, kv, hd = key_cache.shape
    rows_dev, width = queries.shape
    half = width // 2
    group = width // hd // kv
    rows, cols = residual.shape
    keys = key_cache.reshape(batch, ctx * kv, hd)
    values = value_cache.reshape(batch, ctx * kv, hd)
    s = slots(n)
    units = gate_weight.shape[1]
    return pl.pallas_call(
        functools.partial(layer, n),
        out_shape=jax.ShapeDtypeStruct((rows, cols), BF),
        in_specs=[pl.BlockSpec(memory_space=pltpu.SMEM), VM, HBM, HBM, VM, VM, HBM, HBM, HBM, HBM],
        out_specs=VM,
        scratch_shapes=[
            pltpu.VMEM((2, n, rows_dev, half), BF),
            pltpu.VMEM(keys.shape, BF),
            pltpu.VMEM((ctx * kv // 4, hd), F32),
            pltpu.VMEM((batch * kv, ctx, hd), BF),
            pltpu.VMEM((batch * kv, ctx, hd), BF),
            pltpu.VMEM((batch * kv, group * rows // batch, hd), BF),
            pltpu.VMEM((n, rows, width // n), BF),
            pltpu.VMEM((n, rows, width // n), BF),
            pltpu.VMEM((rows, 128), F32),
            pltpu.VMEM((n, 2, 8, rows), F32),
            pltpu.VMEM((n, 2, 8, rows), F32),
            pltpu.VMEM((2, n, rows, hd), BF),
            pltpu.VMEM((2, n, rows, cols // 2), BF),
            pltpu.VMEM((n, 8, rows), F32),
            pltpu.VMEM((2, n, rows, units // 2), BF),
            pltpu.VMEM(out_weight.shape, BF),
            pltpu.VMEM(gate_weight.shape, BF),
            pltpu.VMEM(up_weight.shape, BF),
            pltpu.VMEM(down_weight.shape, BF),
            pltpu.VMEM((rows, cols), F32),
            pltpu.VMEM((rows, cols), F32),
            pltpu.VMEM((rows, units), F32),
            pltpu.VMEM((2, rows, cols), BF),
            pltpu.VMEM((2, rows, cols), BF),
            DMA((2, s)), DMA((2, n)), DMA((batch, n)), DMA((batch, n)), DMA((n,)), DMA((n,)),
            DMA((2, s)), DMA((2, n)), DMA((2, s)), DMA((2, n)), DMA((n,)), DMA((n,)), DMA((n,)),
            DMA((2, s)), DMA((2, n)), DMA((2 + batch,)), DMA((4,)), DMA((2,)), DMA((2,)),
        ],
        compiler_params=pltpu.CompilerParams(
            collective_id=0, has_side_effects=True, vmem_limit_bytes=67_043_328
        ),
        name="layer",
    )(
        lengths, queries, keys, values, residual, norm_gain.reshape(1, -1),
        out_weight, gate_weight, up_weight, down_weight,
    )


def pick(*args):
    queries, key_cache, residual, gate_weight = args[0], args[1], args[4], args[7]
    n = lax.axis_size("blk")
    fits = (
        n == 4 * key_cache.shape[2]
        and queries.shape[0] == 8
        and queries.shape[1] == 256 * n
        and key_cache.shape[3] == 128
        and n % key_cache.shape[0] == 0
        and residual.shape[1] % 256 == 0
        and residual.shape[1] == gate_weight.shape[1]
        and residual.shape[0] == 128
    )
    return kernel_body(*args) if fits else body(*args)


def solution(mesh):
    in_specs = (
        P(("groups", "blk"), "head"),
        P("groups", "blk", "head", None),
        P("groups", "blk", "head", None),
        P("groups"),
        P("groups", "blk"),
        P("head", "blk"),
        P("blk"),
        P(None, ("head", "blk")),
        P(None, ("head", "blk")),
        P("head", "blk"),
    )
    out_specs = P("groups", "blk")
    return jax.shard_map(pick, mesh=mesh, in_specs=in_specs, out_specs=out_specs, check_vma=False)
```

```python
import functools
import math

import jax
import jax.numpy as jnp
from jax import lax
from jax.experimental import pallas as pl
from jax.experimental.pallas import tpu as pltpu
from jax.sharding import PartitionSpec as P

D = 8192


neg_big = -1e30
epsilon = 1e-06


def body(
    queries,
    key_cache,
    value_cache,
    lengths,
    residual,
    out_weight,
    norm_gain,
    gate_weight,
    up_weight,
    down_weight,
):
    blocks = lax.axis_size("blk")
    my_block = lax.axis_index("blk")
    batch, ctx_dev, kv_local, head_dim = key_cache.shape
    rows_dev = queries.shape[0]
    rows_all = rows_dev * blocks
    new_tokens = rows_all // batch
    heads_local = queries.shape[1] // head_dim
    group_size = heads_local // kv_local
    all_queries = lax.all_gather(queries, "blk", axis=0, tiled=True)
    shaped = all_queries.reshape(batch, new_tokens, kv_local, group_size, head_dim)
    scores = jnp.einsum(
        "bqkgd,bckd->bqkgc", shaped, key_cache, preferred_element_type=jnp.float32
    ) * head_dim ** (-0.5)
    query_pos = lengths[:, None] + jnp.arange(new_tokens, dtype=jnp.int32)[None, :]
    key_pos = my_block * ctx_dev + jnp.arange(ctx_dev, dtype=jnp.int32)
    visible = key_pos[None, None, None, None, :] <= query_pos[:, :, None, None, None]
    block_max = jnp.max(jnp.where(visible, scores, neg_big), axis=-1)
    weights = jnp.where(visible, jnp.exp(scores - block_max[..., None]), 0.0)
    block_sum = jnp.sum(weights, axis=-1)
    block_out = jnp.einsum(
        "bqkgc,bckd->bqkgd",
        weights.astype(jnp.bfloat16),
        value_cache,
        preferred_element_type=jnp.float32,
    )
    block_mean = (block_out / jnp.maximum(block_sum, 1.0)[..., None]).astype(jnp.bfloat16)
    row_max = block_max.reshape(rows_all, heads_local)
    row_sum = block_sum.reshape(rows_all, heads_local)
    row_mean = block_mean.reshape(rows_all, heads_local, head_dim)
    got_max, got_sum = (
        lax.all_to_all(row_max[None], "blk", split_axis=1, concat_axis=0, tiled=True),
        lax.all_to_all(row_sum[None], "blk", split_axis=1, concat_axis=0, tiled=True),
    )
    got_mean = lax.all_to_all(row_mean[None], "blk", split_axis=1, concat_axis=0, tiled=True)
    top = jnp.max(got_max, axis=0)
    factor = got_sum * jnp.exp(got_max - top[None])
    total_sum = jnp.sum(factor, axis=0)
    total_out = jnp.sum(got_mean.astype(jnp.float32) * factor[..., None], axis=0)
    attn = (
        (total_out / total_sum[..., None])
        .astype(jnp.bfloat16)
        .reshape(rows_dev, heads_local * head_dim)
    )
    proj_part = jnp.dot(
        lax.all_gather(attn, "blk", axis=0, tiled=True),
        out_weight,
        preferred_element_type=jnp.float32,
    )
    projected = lax.psum(proj_part.astype(jnp.bfloat16), "head").astype(jnp.float32)
    stream = residual.astype(jnp.float32) + projected
    squares = lax.psum(jnp.sum(stream * stream, axis=1), "blk")
    normed = (
        stream * lax.rsqrt(squares / D + epsilon)[:, None] * norm_gain.astype(jnp.float32)[None, :]
    ).astype(jnp.bfloat16)
    piece = lax.all_gather(normed, "blk", axis=1, tiled=True)
    gate = jnp.dot(piece, gate_weight, preferred_element_type=jnp.float32)
    up = jnp.dot(piece, up_weight, preferred_element_type=jnp.float32)
    hidden = (jax.nn.silu(gate) * up).astype(jnp.bfloat16)
    down_part = jnp.dot(
        lax.all_gather(hidden, "blk", axis=1, tiled=True),
        down_weight,
        preferred_element_type=jnp.float32,
    )
    down_total = lax.psum(down_part.astype(jnp.bfloat16), "head").astype(jnp.float32)
    return (stream + down_total).astype(jnp.bfloat16)


MESH = pl.DeviceIdType.MESH
BF = jnp.bfloat16
F32 = jnp.float32


def remote(src, dst, ssem, rsem, **where):
    return pltpu.make_async_remote_copy(
        src_ref=src, dst_ref=dst, send_sem=ssem, recv_sem=rsem, device_id=where, device_id_type=MESH
    )


def enter(n, me, head):
    barrier = pltpu.get_barrier_semaphore()
    for k in range(1, n):
        pl.semaphore_signal(
            barrier, inc=1, device_id={"blk": lax.rem(me + k, n)}, device_id_type=MESH
        )
    pl.semaphore_signal(barrier, inc=1, device_id={"head": 1 - head}, device_id_type=MESH)
    pl.semaphore_wait(barrier, n)


def start_if(cond, copy):
    if cond is None:
        copy.start()
    else:
        pl.when(cond)(copy.start)


def gather(buf, parts, ssem, rsem, n, me, forward=None, work=(), visit=None):
    depth = n // 4
    z = me // 4
    x_peer = me + 1 - 2 * (me % 2)
    y_peer = me + 2 - 4 * ((me // 2) % 2)
    sends = []

    def send(part, slot, block, target, cond=None):
        copy = remote(
            buf.at[part, block], buf.at[part, block], ssem.at[part, slot], rsem.at[part, block], blk=target
        )
        start_if(cond, copy)
        sends.append((cond, copy))

    def pass_on(part, block, cond=None):
        if forward is not None:
            head, fsem = forward
            copy = remote(
                buf.at[part, block], buf.at[part, block], fsem.at[block], rsem.at[part, block], head=1 - head
            )
            start_if(cond, copy)
            sends.append((cond, copy))

    def arrived(part, block, cond=None):
        copy = remote(
            buf.at[part, block], buf.at[part, block], ssem.at[part, 0], rsem.at[part, block], blk=x_peer
        )
        if cond is None:
            copy.wait_recv()
        else:
            pl.when(cond)(copy.wait_recv)

    def peers(first):
        return x_peer * (1 - first) + y_peer * first, y_peer * (1 - first) + x_peer * first

    for part, first in parts:
        near, far = peers(first)
        send(part, 0, me, me + 4, z < depth - 1)
        send(part, 1, me, me - 4, z > 0)
        send(part, 2, me, near)
        send(part, 3, me, far)
        pass_on(part, me)
    work = list(work)
    if work:
        work.pop(0)()
    slot = 4
    for d in range(1, depth):
        for step in (4, -4):
            for part, first in parts:
                near, far = peers(first)
                block = me - step * d
                if step > 0:
                    here = z >= d
                    more = jnp.logical_and(z >= d, z < depth - 1)
                else:
                    here = z < depth - d
                    more = jnp.logical_and(z < depth - d, z > 0)
                arrived(part, block, here)
                send(part, slot, block, me + step, more)
                send(part, slot + 1, block, near, here)
                send(part, slot + 2, block, far, here)
                pass_on(part, block, here)
            slot += 3
        if work:
            work.pop(0)()
    for k in range(depth):
        zz = lax.rem(z + k, depth)
        for part, first in parts:
            near, far = peers(first)
            block = near + 4 * (zz - z)
            arrived(part, block)
            send(part, slot, block, far)
            pass_on(part, block)
        slot += 1
    if work:
        work.pop(0)()
    others = [] if forward is None else [(1 - p, 1 - f) for p, f in parts]
    for group in (parts, others):
        items = []
        for k in range(depth):
            shift = 4 * (lax.rem(z + k, depth) - z)
            for part, first in group:
                near, far = peers(first)
                if group is others:
                    arrived(part, me + shift)
                    arrived(part, near + shift)
                items += [(part, me + shift), (part, near + shift)]
        if visit is not None and items:
            visit(items)
    for k in range(depth):
        shift = 4 * (lax.rem(z + k, depth) - z)
        items = []
        for mine, (part, first) in [(True, p) for p in parts] + [(False, p) for p in others]:
            near, far = peers(first)
            for block in (far + shift, near + far - me + shift):
                arrived(part, block)
                if mine:
                    pass_on(part, block)
                items.append((part, block))
        if visit is not None:
            visit(items)

    def finish():
        for cond, copy in sends:
            if cond is None:
                copy.wait_send()
            else:
                pl.when(cond)(copy.wait_send)

    return finish


def slots(n):
    depth = n // 4
    return 4 + 6 * (depth - 1) + depth


def swap(part, mine, theirs, ssem, rsem, head):
    mine[...] = part.astype(BF)
    copy = remote(mine, theirs, ssem, rsem, head=1 - head)
    copy.start()
    copy.wait()
    return mine[...].astype(F32) + theirs[...].astype(F32)


def layer(
    n, lengths, q, keys, values, residual, gain, ow, gw, uw, dw, out,
    qbuf, raw, wide, kd, vd, qs, osend, orecv, stat, ssend, srecv, abuf, sbuf, sqbuf, hbuf,
    ow_v, gv, uv, dv, stream, acc, gacc, mine, theirs,
    gss, qrs, oss, ors, tss, trs, ars, srs, nrs, hrs, loc, wsem, xss, xrs,
):
    me = lax.axis_index("blk")
    head = lax.axis_index("head")
    batch, flat, hd = raw.shape
    kv = kd.shape[0] // batch
    ctx = flat // kv
    rows_dev, width = q.shape
    half = width // 2
    per = half // hd
    group = width // hd // kv
    owners = n // batch
    tokens = owners * rows_dev
    rows = batch * tokens
    wcopies = [
        pltpu.make_async_copy(a, b, wsem.at[i])
        for i, (a, b) in enumerate(((ow, ow_v), (gw, gv), (uw, uv), (dw, dv)))
    ]
    qcopies = [
        pltpu.make_async_copy(q.at[:, pl.ds(p * half, half)], qbuf.at[p, me], loc.at[p]) for p in range(2)
    ]
    for c in qcopies:
        c.start()
    kcopies = [pltpu.make_async_copy(keys.at[b], raw.at[b], loc.at[2 + b]) for b in range(batch)]
    vcopies = [pltpu.make_async_copy(values.at[b], raw.at[b], loc.at[2 + b]) for b in range(batch)]
    for c in kcopies:
        c.start()
    enter(n, me, head)
    for c in qcopies:
        c.wait()

    def spread_heads(dest, b, copies, after):
        def run():
            copies[b].wait()
            part = wide.shape[0]
            for c in range(flat // part):
                wide[...] = raw[b, c * part : (c + 1) * part].astype(F32)
                for h in range(kv):
                    dest[b * kv + h, c * part // kv : (c + 1) * part // kv] = wide[
                        pl.ds(h, part // kv, stride=kv), :
                    ].astype(BF)
            for c in after:
                c.start()
        return run

    jobs = []
    for b in range(batch):
        jobs.append(spread_heads(kd, b, kcopies, [vcopies[b]]))
    for b in range(batch):
        jobs.append(spread_heads(vd, b, vcopies, wcopies if b == batch - 1 else []))
    finish_q = gather(qbuf, [(0, 0), (1, 1)], gss, qrs, n, me, work=jobs)
    for b in range(batch):
        for j in range(kv * group):
            val = qbuf[j // per, b * owners : (b + 1) * owners, :, (j % per) * hd : (j % per + 1) * hd]
            val = val.astype(F32).reshape(tokens, hd).astype(BF)
            h, g = j // group, j % group
            qs[b * kv + h, g * tokens : (g + 1) * tokens] = val
    scale = hd ** (-0.5) * math.log2(math.e)
    gt = 4
    tile = gt * tokens
    share = n // kv
    heads_each = group // share
    lane = lax.broadcasted_iota(jnp.int32, (tokens, 128), 1)
    z = me // 4

    def one(b, h):
        bh = b * kv + h
        limit = lengths[b] - me * ctx
        first_row = pl.multiple_of(b * tokens, tokens)
        stats = jnp.zeros((tokens, 128), F32)
        for rt in range(group // gt):
            s = lax.dot_general(
                qs[bh, rt * tile : (rt + 1) * tile], kd[bh], (((1,), (1,)), ((), ())), preferred_element_type=F32
            ) * scale
            row = lax.broadcasted_iota(jnp.int32, (tile, 1), 0) % tokens
            col = lax.broadcasted_iota(jnp.int32, (tile, ctx), 1)
            s = jnp.where(col <= row + limit, s, neg_big)
            m = jnp.max(s, axis=1, keepdims=True)
            p = jnp.exp2(s - jnp.maximum(m, -1e29))
            l = jnp.sum(p, axis=1, keepdims=True)
            o = jnp.dot(p.astype(BF), vd[bh], preferred_element_type=F32)
            o = (o / jnp.maximum(l, 1.0)).astype(BF)
            for g in range(gt):
                j, e = divmod(rt * gt + g, heads_each)
                cut = slice(g * tokens, (g + 1) * tokens)
                osend[h * share + j, pl.ds(first_row, tokens), e * hd : (e + 1) * hd] = o[cut]
                stats = jnp.where(lane == j * 8 + e, m[cut], stats)
                stats = jnp.where(lane == 64 + j * 8 + e, l[cut], stats)
            for j in range(rt * gt // heads_each, (rt + 1) * gt // heads_each):
                to = h * share + j
                copy = remote(
                    osend.at[to, pl.ds(first_row, tokens)], orecv.at[me, pl.ds(first_row, tokens)],
                    oss.at[b, to], ors.at[b, me], blk=to,
                )
                start_if(to != me, copy)
        stat[pl.ds(first_row, tokens)] = stats

    def plane(k, carry):
        h = lax.rem(z + kv - 1 - k, kv)

        def each(b, c):
            one(b, h)
            return c

        lax.fori_loop(0, batch, each, 0)
        turned = stat[...].T
        for j in range(share):
            to = h * share + j
            for which in range(2):
                ssend[to, which] = turned[which * 64 + j * 8 : which * 64 + j * 8 + 8]
            start_if(to != me, remote(ssend.at[to], srecv.at[me], tss.at[to], trs.at[me], blk=to))
        return carry

    lax.fori_loop(0, kv, plane, 0)
    own = [
        pltpu.make_async_copy(ssend.at[me], srecv.at[me], loc.at[0]),
        pltpu.make_async_copy(osend.at[me], orecv.at[me], loc.at[1]),
    ]
    for c in own:
        c.start()
    finish_q()
    for c in own:
        c.wait()
    for i in range(n):
        for b in range(batch):
            cut = pl.ds(b * tokens, tokens)
            copy = remote(osend.at[i, cut], orecv.at[i, cut], oss.at[b, i], ors.at[b, i], blk=i)
            pl.when(i != me)(copy.wait)
        pl.when(i != me)(remote(ssend.at[i], srecv.at[i], tss.at[i], trs.at[i], blk=i).wait)
    maxima = srecv[:, 0]
    top = jnp.max(maxima, axis=0)
    factor = srecv[:, 1] * jnp.exp2(maxima - top[None])
    ratio = (factor / jnp.sum(factor, axis=0)[None]).reshape(n * 8, rows).T
    for e in range(heads_each):
        total = jnp.zeros((rows, hd), F32)
        for i in range(n):
            total += orecv[i, :, e * hd : (e + 1) * hd].astype(F32) * ratio[:, i * 8 + e : i * 8 + e + 1]
        abuf[e, me] = total.astype(BF)

    def products(buf, pairs):
        cut = buf.shape[3]

        def visit(items):
            for c in range(0, len(items), 4):
                for total, w in pairs:
                    term = total[...]
                    for part, block in items[c : c + 4]:
                        at = pl.multiple_of(block * (2 * cut) + part * cut, cut)
                        term += jnp.dot(buf[part, block], w[pl.ds(at, cut), :], preferred_element_type=F32)
                    total[...] = term
        return visit

    acc[...] = jnp.zeros_like(acc)
    for c in wcopies:
        c.wait()
    finish_a = gather(abuf, [(0, 0), (1, 1)], gss, ars, n, me, visit=products(abuf, ((acc, ow_v),)))
    new = residual[...].astype(F32) + swap(acc[...], mine.at[0], theirs.at[0], xss.at[0], xrs.at[0], head)
    stream[...] = new
    scaled = (new * gain[...].astype(F32)).astype(BF)
    cut = scaled.shape[1] // 2
    for p in range(2):
        sbuf[p, me] = scaled[:, p * cut : (p + 1) * cut]
    sqbuf[me] = lax.dot_general(
        jnp.ones((8, new.shape[1]), F32), new * new, (((1,), (1,)), ((), ())),
        precision=lax.Precision.HIGHEST, preferred_element_type=F32,
    )
    acc[...] = jnp.zeros_like(acc)
    gacc[...] = jnp.zeros_like(gacc)
    finish_a()
    for i in range(n):
        start_if(i != me, remote(sqbuf.at[me], sqbuf.at[me], tss.at[i], nrs.at[me], blk=i))
    finish_s = gather(
        sbuf, [(0, 0), (1, 1)], gss, srs, n, me,
        visit=products(sbuf, ((gacc, gv), (acc, uv))),
    )
    for i in range(n):
        pl.when(i != me)(remote(sqbuf.at[i], sqbuf.at[i], tss.at[i], nrs.at[i], blk=i).wait)
    spread = lax.dot_general(
        jnp.sum(sqbuf[...], axis=0), jnp.full((8, gacc.shape[1]), 0.125, F32), (((0,), (0,)), ((), ())),
        precision=lax.Precision.HIGHEST, preferred_element_type=F32,
    )
    norm = lax.rsqrt(spread / (n * stream.shape[1]) + epsilon)
    gate = gacc[...] * norm
    hidden = ((gate / (1.0 + jnp.exp(-gate))) * (acc[...] * norm)).astype(BF)
    cut = hidden.shape[1] // 2
    hbuf[0, me] = hidden[:, :cut]
    hbuf[1, me] = hidden[:, cut:]
    acc[...] = jnp.zeros_like(acc)
    finish_s()
    finish_h = gather(hbuf, [(0, 0), (1, 1)], gss, hrs, n, me, visit=products(hbuf, ((acc, dv),)))
    down = swap(acc[...], mine.at[1], theirs.at[1], xss.at[1], xrs.at[1], head)
    out[...] = (stream[...] + down).astype(BF)
    finish_h()


VM = pl.BlockSpec(memory_space=pltpu.VMEM)
HBM = pl.BlockSpec(memory_space=pl.ANY)
DMA = pltpu.SemaphoreType.DMA


def kernel_body(
    queries, key_cache, value_cache, lengths, residual, out_weight, norm_gain, gate_weight, up_weight, down_weight
):
    n = lax.axis_size("blk")
    batch, ctx, kv, hd = key_cache.shape
    rows_dev, width = queries.shape
    half = width // 2
    group = width // hd // kv
    rows, cols = residual.shape
    keys = key_cache.reshape(batch, ctx * kv, hd)
    values = value_cache.reshape(batch, ctx * kv, hd)
    s = slots(n)
    units = gate_weight.shape[1]
    return pl.pallas_call(
        functools.partial(layer, n),
        out_shape=jax.ShapeDtypeStruct((rows, cols), BF),
        in_specs=[pl.BlockSpec(memory_space=pltpu.SMEM), VM, HBM, HBM, VM, VM, HBM, HBM, HBM, HBM],
        out_specs=VM,
        scratch_shapes=[
            pltpu.VMEM((2, n, rows_dev, half), BF),
            pltpu.VMEM(keys.shape, BF),
            pltpu.VMEM((ctx * kv // 4, hd), F32),
            pltpu.VMEM((batch * kv, ctx, hd), BF),
            pltpu.VMEM((batch * kv, ctx, hd), BF),
            pltpu.VMEM((batch * kv, group * rows // batch, hd), BF),
            pltpu.VMEM((n, rows, width // n), BF),
            pltpu.VMEM((n, rows, width // n), BF),
            pltpu.VMEM((rows, 128), F32),
            pltpu.VMEM((n, 2, 8, rows), F32),
            pltpu.VMEM((n, 2, 8, rows), F32),
            pltpu.VMEM((2, n, rows, hd), BF),
            pltpu.VMEM((2, n, rows, cols // 2), BF),
            pltpu.VMEM((n, 8, rows), F32),
            pltpu.VMEM((2, n, rows, units // 2), BF),
            pltpu.VMEM(out_weight.shape, BF),
            pltpu.VMEM(gate_weight.shape, BF),
            pltpu.VMEM(up_weight.shape, BF),
            pltpu.VMEM(down_weight.shape, BF),
            pltpu.VMEM((rows, cols), F32),
            pltpu.VMEM((rows, cols), F32),
            pltpu.VMEM((rows, units), F32),
            pltpu.VMEM((2, rows, cols), BF),
            pltpu.VMEM((2, rows, cols), BF),
            DMA((2, s)), DMA((2, n)), DMA((batch, n)), DMA((batch, n)), DMA((n,)), DMA((n,)),
            DMA((2, n)), DMA((2, n)), DMA((n,)), DMA((2, n)),
            DMA((2 + batch,)), DMA((4,)), DMA((2,)), DMA((2,)),
        ],
        compiler_params=pltpu.CompilerParams(
            collective_id=0, has_side_effects=True, vmem_limit_bytes=67_043_328
        ),
        name="layer",
    )(
        lengths, queries, keys, values, residual, norm_gain.reshape(1, -1),
        out_weight, gate_weight, up_weight, down_weight,
    )


def pick(*args):
    queries, key_cache, residual, gate_weight = args[0], args[1], args[4], args[7]
    n = lax.axis_size("blk")
    fits = (
        n == 4 * key_cache.shape[2]
        and queries.shape[0] == 8
        and queries.shape[1] == 256 * n
        and key_cache.shape[3] == 128
        and n % key_cache.shape[0] == 0
        and residual.shape[1] % 256 == 0
        and residual.shape[1] == gate_weight.shape[1]
        and residual.shape[0] == 128
    )
    return kernel_body(*args) if fits else body(*args)


def solution(mesh):
    in_specs = (
        P(("groups", "blk"), "head"),
        P("groups", "blk", "head", None),
        P("groups", "blk", "head", None),
        P("groups"),
        P("groups", "blk"),
        P("head", "blk"),
        P("blk"),
        P(None, ("head", "blk")),
        P(None, ("head", "blk")),
        P("head", "blk"),
    )
    out_specs = P("groups", "blk")
    return jax.shard_map(pick, mesh=mesh, in_specs=in_specs, out_specs=out_specs, check_vma=False)
```
